32 devices in a mesh: region: 16 (over z, y, x), mp: 2 (over core).
Axes of the slice: x: 2, y: 2, z: 4, core: 2. Of those that a mesh axis runs over, the one named last changes fastest.
Arguments:
- grid: bfloat16 [32768, 1024], P('region', 'mp'), may hold values from -6 to 6
- g2m_weight: float32 [32768], P('region'), may hold values from 0.3 to 1
- g2m_slot: int32 [32768], P('region'), may hold values from 0 to 511
- slot_node: int32 [16, 16, 32], P('region'), may hold values from 0 to 511, as said below
- peer_mask: int32 [16, 4], P('region'), may hold values 0 or 1
- norm_gain: float32 [1024], replicated, may hold values from 0.25 to 1.75
- w_qkv: bfloat16 [3, 1024, 1024], P(None, None, 'mp')
- w_out: bfloat16 [1024, 1024], P('mp'), may hold values from -0.1875 to 0.1875
Outputs:
- mesh_state: float32 [8192, 1024], P('region', 'mp')
- grid_out: bfloat16 [32768, 1024], P('region', 'mp')
The draws below stay inside these ranges and needn't reach their ends.
Inputs may be any that keep to these rules, and one draw needn't show every extreme that they name: `slot_node`: for each mesh tile o and lane c, the entries over all grid tiles r lie in one range b * (16) to (b + 1) * 16 - 1 and name every node of that range, where the range b depends on o and c and different lanes of one mesh tile take different ranges; so every mesh node is named by some send slot, and the 32 slots of one grid tile for one mesh tile name different nodes.
All inputs are finite; a program needn't handle non-finite values. No bound on the sum of `peer_mask` on one device may be relied on, other than what follows from the above.
Results may differ from the reference program's by a relative error of at most 0.006.
Values may be sent and summed in bfloat16 or wider, within the bound.
A program may use at most 192 MiB of HBM per device.

```python
import math
import jax
import jax.numpy as jnp
from jax import lax

D = 1024
HEADS = 16
HEAD_DIM = 64
MESH_DEV = 512
GRID_DEV = 2048
SEND_SLOTS = 512
GRID = 32768
N_REGION = 16


def draw_slot_node(key, part):
    cap = SEND_SLOTS // N_REGION
    stride = MESH_DEV // cap
    keys = jax.random.split(jax.random.fold_in(key, 17), N_REGION * cap)
    orders = jax.vmap(lambda k: jax.random.permutation(k, N_REGION))(keys).astype(jnp.int32)
    orders = orders.reshape(N_REGION, cap, N_REGION)
    lane_keys = jax.random.split(jax.random.fold_in(key, 23), N_REGION)
    ranges = jax.vmap(lambda k: jax.random.permutation(k, cap))(lane_keys).astype(jnp.int32)
    table = orders % stride + ranges[:, :, None] * stride
    return jnp.transpose(table, (0, 2, 1)).astype(jnp.int32)


def draw_w_qkv(key, part):
    first = jax.random.fold_in(jax.random.fold_in(key, 29), 0)
    base = jax.random.normal(first, (3, D, D), jnp.float32) * D ** (-0.5)
    return base.astype(jnp.bfloat16)


def place_ends(array, own_key, least, largest):
    extent = array.shape
    place = [jax.random.randint(jax.random.fold_in(own_key, axis), (), 0, extent[axis]) for axis in range(len(extent))]
    array = array.at[tuple(place)].set(least)
    longest = extent.index(max(extent))
    place[longest] = (place[longest] + 1) % extent[longest]
    return array.at[tuple(place)].set(largest)


def shard_levels(rng, shape, cuts, least, top_value):
    def one(dim, parts):
        heights = jax.random.uniform(jax.random.fold_in(jax.random.fold_in(rng, 6), dim), (parts,), jnp.float32, least / len(cuts), top_value / len(cuts))
        return jnp.repeat(jnp.exp(heights), shape[dim] // parts).reshape((-1,) + (1,) * (len(shape) - dim - 1))

    loudness = one(*cuts[0])
    for cut in cuts[1:]:
        loudness = loudness * one(*cut)
    return loudness


def centred(stream_key, extent, scale, limit, pieces=(), kind=jnp.bfloat16):
    loudness = shard_levels(stream_key, extent, pieces, -0.22, 0.18) if pieces else 1.0
    entries = jax.random.normal(stream_key, extent, jnp.float32) * scale * loudness
    return jnp.minimum(jnp.maximum(entries, -limit), limit).astype(kind)


def setup_inputs(seed: int = 0) -> dict:
    streams_of = jax.random.split(jax.random.key(seed), 9)
    return {
        "grid": centred(streams_of[0], (GRID, D), 1.0, 6.0, ((0, 16), (1, 2))),
        "g2m_weight": jnp.clip(jnp.exp(math.log(1.0) - 1.2039728 * jax.random.uniform(streams_of[1], (GRID,), jnp.float32) ** shard_levels(streams_of[1], (GRID,), ((0, 16),), -0.2, 0.2)), 0.3, 1.0),
        "g2m_slot": place_ends(jax.random.randint(streams_of[2], (GRID,), 0, SEND_SLOTS), jax.random.fold_in(streams_of[2], 1), 0, SEND_SLOTS - 1).astype(jnp.int32),
        "slot_node": draw_slot_node(jax.random.fold_in(streams_of[8], 71), 0),
        "peer_mask": place_ends((jax.random.randint(streams_of[4], (N_REGION, 4), 0, 4) < 3).astype(jnp.int32), jax.random.fold_in(streams_of[4], 1), 0, 1),
        "norm_gain": jnp.clip(1.0 + 0.15 * jax.random.normal(streams_of[5], (D,), jnp.float32), 0.25, 1.75),
        "w_qkv": draw_w_qkv(jax.random.fold_in(streams_of[8], 71), 0),
        "w_out": centred(streams_of[7], (D, D), D ** -0.5, 0.1875, ((0, 2),)),
    }


OFFSETS = (-2, -1, 1, 2)

def reference(grid, g2m_weight, g2m_slot, slot_node, peer_mask, norm_gain, w_qkv, w_out):
    regions = N_REGION
    cap = SEND_SLOTS // N_REGION
    scaled = (g2m_weight[:, None] * grid.astype(jnp.float32)).astype(jnp.bfloat16)
    scaled = scaled.reshape(regions, GRID_DEV, D)
    slot_tiles = g2m_slot.reshape(regions, GRID_DEV).astype(jnp.int32)

    def tile_partial(pair):
        values, slots = pair
        onehot = (slots[None, :] == jnp.arange(SEND_SLOTS, dtype=jnp.int32)[:, None]).astype(jnp.bfloat16)
        return jnp.dot(onehot, values, preferred_element_type=jnp.float32).astype(jnp.bfloat16)
    partial_value = lax.map(tile_partial, (scaled, slot_tiles))
    owners = jnp.arange(SEND_SLOTS, dtype=jnp.int32) // cap
    by_grid = jnp.transpose(slot_node, (1, 0, 2)).reshape(regions, SEND_SLOTS).astype(jnp.int32)
    node_table = (owners[None, :] * MESH_DEV + by_grid).astype(jnp.int32)
    mesh_in = jax.ops.segment_sum(partial_value.reshape(-1, D).astype(jnp.float32), node_table.reshape(-1), num_segments=MESH_DEV * regions)
    mesh_low = lax.optimization_barrier(mesh_in.astype(jnp.bfloat16)).astype(jnp.float32)
    normed = (mesh_low * lax.rsqrt(lax.optimization_barrier(jnp.mean(mesh_low * mesh_low, axis=-1, keepdims=True)) + 1e-05) * norm_gain).astype(jnp.bfloat16)
    queries = jnp.dot(normed, w_qkv[0], preferred_element_type=jnp.float32).astype(jnp.bfloat16)
    keys = jnp.dot(normed, w_qkv[1], preferred_element_type=jnp.float32).astype(jnp.bfloat16)
    values = jnp.dot(normed, w_qkv[2], preferred_element_type=jnp.float32).astype(jnp.bfloat16)
    q_tiles = queries.reshape(regions, MESH_DEV, HEADS, HEAD_DIM)
    k_tiles = keys.reshape(regions, MESH_DEV, HEADS, HEAD_DIM)
    v_tiles = values.reshape(regions, MESH_DEV, HEADS, HEAD_DIM)

    def tile_attend(tile):
        order = [tile] + [(tile + offset) % regions for offset in OFFSETS]
        key_block = jnp.concatenate([k_tiles[index] for index in order], axis=0)
        val_block = jnp.concatenate([v_tiles[index] for index in order], axis=0)
        active = jnp.concatenate([jnp.ones((1,), jnp.int32), peer_mask[tile].astype(jnp.int32)])
        valid = jnp.repeat(active, MESH_DEV)
        scores = jnp.einsum('qhd,khd->hqk', q_tiles[tile].astype(jnp.float32), key_block.astype(jnp.float32)) * HEAD_DIM ** (-0.5)
        scores = jnp.where(valid[None, None, :] > 0, scores, -1e+30)
        top = lax.optimization_barrier(jnp.max(scores, axis=-1, keepdims=True))
        expd = jnp.exp(scores - top)
        weights = (expd / lax.optimization_barrier(jnp.sum(expd, axis=-1, keepdims=True))).astype(jnp.bfloat16)
        out = jnp.einsum('hqk,khd->qhd', weights.astype(jnp.float32), val_block.astype(jnp.float32))
        return out.astype(jnp.bfloat16).reshape(MESH_DEV, D)
    attended = lax.map(tile_attend, jnp.arange(regions, dtype=jnp.int32)).reshape(-1, D)
    mesh_state = mesh_in + jnp.dot(attended, w_out, preferred_element_type=jnp.float32)
    mesh_back = mesh_state.astype(jnp.bfloat16)
    point_nodes = jnp.take_along_axis(node_table, slot_tiles, axis=1).reshape(-1)
    grid_out = (grid.astype(jnp.float32) + mesh_back[point_nodes].astype(jnp.float32)).astype(jnp.bfloat16)
    return (mesh_state, grid_out)
```

```python
import functools

import jax
import jax.numpy as jnp
from jax import lax
from jax.experimental import pallas as pl
from jax.experimental.pallas import tpu as pltpu
from jax.sharding import PartitionSpec as P

HEAD_DIM = 64
PAD = 80
PEERS = 4
Y, NEAR, RELAYED, Z = range(PEERS)
MESH = pl.DeviceIdType.MESH
LOG2E = 1.4426950408889634
NT = (((1,), (1,)), ((), ()))


def window_kernel(
    n, mp, grid_ref, weight_ref, slot_ref, node_ref, peer_ref, gain_ref, w_ref, wo_ref,
    mesh_ref, returned_ref,
    points, wcol, scaled, part, xg, gath, wbuf, wobuf, wvt, hot, rowm, colm,
    qm, kown, kbuf, vbuf, sbuf, acc, top, attb, out_part, in_part, total, state, back, ordered,
    local, gsem, wsem, asend, arecv, xsend, xrecv, psend, precv, msend, mrecv, rsend, rrecv,
    bsend, brecv,
):
    f32, bf16 = jnp.float32, jnp.bfloat16
    region = lax.axis_index("region")
    core = lax.axis_index("mp")
    count, width = points.shape
    rows = xg.shape[1]
    cap = rows // n
    heads = width // HEAD_DIM
    peers = PEERS
    chunk = rows // peers
    blocks = 1 + peers
    half = rows // 2
    piece = count // peers
    odd = lax.rem(region, 2)
    far = lax.rem(region // 2, 2)
    step = 2 - 4 * odd
    partner = region + 1 - 2 * odd
    across = region + 2 - 4 * far
    beyond = lax.rem(region + 4 - 8 * far + n, n)
    second = lax.rem(region + step + n, n)
    relay_place = jnp.where(odd == far, Y, Z)
    cols = pl.ds(pl.multiple_of(core * width, width), width)

    loads = [
        pltpu.make_async_copy(
            grid_ref.at[pl.ds(k * piece, piece)], points.at[pl.ds(k * piece, piece)], gsem.at[k]
        )
        for k in range(peers)
    ]
    for load in loads:
        load.start()
    weights = [
        pltpu.make_async_copy(w_ref, wbuf, wsem.at[0]),
        pltpu.make_async_copy(wo_ref, wobuf, wsem.at[1]),
    ]
    for load in weights:
        load.start()

    barrier = pltpu.get_barrier_semaphore()

    def hello(d, carry):
        pl.semaphore_signal(
            barrier, inc=1, device_id={"region": lax.rem(region + d, n)}, device_id_type=MESH
        )
        return carry

    lax.fori_loop(1, n, hello, 0)
    for j in range(1, mp):
        pl.semaphore_signal(
            barrier, inc=1, device_id={"mp": lax.rem(core + j, mp)}, device_id_type=MESH
        )

    wcol[...] = jnp.broadcast_to(weight_ref[...], (8, count)).T
    for k in range(peers):
        loads[k].wait()
        span = slice(k * piece, (k + 1) * piece)
        scaled[span] = (wcol[span, 0:1] * points[span].astype(f32)).astype(bf16)

    def mine_of(ref):
        return ref.at[pl.ds(pl.multiple_of(region * cap, cap), cap)]

    def base_of(j):
        return region + n // 4 + j * (n // 2)

    def scatter(j):
        place = lax.broadcasted_iota(jnp.int32, (half, 1), 0)
        ids = lax.rem(place // cap + base_of(j), n) * cap + lax.rem(place, cap)
        part[j] = jnp.dot(
            jnp.where(ids == slot_ref[...], 1.0, 0.0).astype(bf16),
            scaled[...],
            preferred_element_type=f32,
        ).astype(bf16)

    def sow(j, k):
        return pltpu.make_async_remote_copy(
            src_ref=part.at[j, pl.ds(pl.multiple_of(k * cap, cap), cap)],
            dst_ref=mine_of(xg.at[core]),
            send_sem=asend.at[j * (n // 2) + k],
            recv_sem=arecv.at[region],
            device_id={"region": lax.rem(base_of(j) + k, n)},
            device_id_type=MESH,
        )

    def sow_all(j, lo, hi):
        def go(k, carry):
            sow(j, k).start()
            return carry

        lax.fori_loop(lo, hi, go, 0)

    scatter(0)
    pl.semaphore_wait(barrier, n - 1 + mp - 1)
    sow_all(0, 0, n // 2)
    scatter(1)
    sow_all(1, 0, n // 4)
    sow_all(1, n // 4 + 1, n // 2)
    own = pltpu.make_async_copy(
        part.at[1, pl.ds(n // 4 * cap, cap)], mine_of(xg.at[core]), local.at[0]
    )
    own.start()

    acc[...] = jnp.zeros_like(acc)
    top[...] = jnp.full_like(top, -1e30)
    seen = [peer_ref[0, i].astype(f32) for i in range(4)]
    shown = {
        Y: jnp.where(far == 0, seen[3], seen[0]),
        Z: jnp.where(far == 0, seen[0], seen[3]),
        NEAR: jnp.where(odd == 0, seen[2], seen[1]),
        RELAYED: jnp.where(odd == 0, seen[1], seen[2]),
    }
    for ref, axis in ((rowm, 1), (colm, 0)):
        shape = ref.shape[1:]
        place = lax.broadcasted_iota(jnp.int32, shape, axis) // chunk
        mask = jnp.zeros(shape, f32)
        for p in range(peers):
            mask = jnp.where(place == p, shown[p], mask)
        ref[0] = jnp.ones(shape, f32)
        ref[1] = mask
    lane = lax.broadcasted_iota(jnp.int32, (n, rows), 1)
    spread = jnp.zeros((n, rows), jnp.int32)
    for c in range(cap):
        spread = jnp.where(lax.rem(lane, cap) == c, node_ref[0, :, c : c + 1], spread)
    owner = lax.broadcasted_iota(jnp.int32, (n, rows), 0)
    flat = jnp.sum(jnp.where(lane // cap == owner, spread, 0), axis=0, keepdims=True)
    hot[...] = jnp.where(
        lax.broadcasted_iota(jnp.int32, (rows, rows), 0) == flat, 1.0, 0.0
    ).astype(bf16)
    for load in weights:
        load.wait()
    wvt[...] = wbuf[2].T
    own.wait()

    def x_to_core(q, j):
        span = pl.ds(pl.multiple_of(q * chunk, chunk), chunk)
        return pltpu.make_async_remote_copy(
            src_ref=xg.at[core, span],
            dst_ref=xg.at[core, span],
            send_sem=xsend.at[q, j],
            recv_sem=xrecv.at[q, j],
            device_id={"mp": lax.rem(core + j, mp)},
            device_id_type=MESH,
        )

    def reaped(q, carry):
        def one(k, c):
            source = q * (n // peers) + k

            @pl.when(source != region)
            def _():
                pltpu.make_async_remote_copy(
                    src_ref=part.at[0, pl.ds(0, cap)],
                    dst_ref=xg.at[core, pl.ds(pl.multiple_of(source * cap, cap), cap)],
                    send_sem=asend.at[0],
                    recv_sem=arecv.at[source],
                    device_id={"region": partner},
                    device_id_type=MESH,
                ).wait_recv()

            return c

        lax.fori_loop(0, n // peers, one, 0)
        for j in range(1, mp):
            x_to_core(q, j).start()
        return carry

    lax.fori_loop(0, peers, reaped, 0)

    def send(c, place, source, other):
        return pltpu.make_async_remote_copy(
            src_ref=source,
            dst_ref=gath.at[1 + c, pl.ds(place * chunk, chunk), cols],
            send_sem=psend.at[c, place],
            recv_sem=precv.at[c, place],
            device_id={"region": other},
            device_id_type=MESH,
        )

    def own_chunk(c):
        return gath.at[0, pl.ds(pl.multiple_of(c * chunk, chunk), chunk), cols]

    def held(c, place):
        return gath.at[1 + c, pl.ds(pl.multiple_of(place * chunk, chunk), chunk), cols]

    def to_near(c):
        return send(c, NEAR, own_chunk(c), partner)

    def to_across(c):
        return send(c, Y, own_chunk(c), across)

    def forward(c):
        return send(c, Z, held(c, Y), beyond)

    def relay(c):
        if c % 2 == 0:
            return send(c, RELAYED, held(c, NEAR), second)
        return send(c, RELAYED, held(c, relay_place), partner)

    def arrived(c, place):
        pltpu.make_async_remote_copy(
            src_ref=own_chunk(0),
            dst_ref=held(c, place),
            send_sem=psend.at[c, place],
            recv_sem=precv.at[c, place],
            device_id={"region": partner},
            device_id_type=MESH,
        ).wait_recv()

    def normalise(q, carry):
        for j in range(1, mp):
            x_to_core(q, j).wait_recv()
        span = pl.ds(pl.multiple_of(q * chunk, chunk), chunk)
        square = jnp.zeros((chunk, 1), f32)
        for m in range(mp):
            value = xg[m, span].astype(f32)
            square += jnp.sum(value * value, axis=-1, keepdims=True)
        inv = lax.rsqrt(square / (mp * width) + 1e-05)
        for m in range(mp):
            at = slice(m * width, (m + 1) * width)
            gath[0, span, at] = (xg[m, span].astype(f32) * inv * gain_ref[:, at]).astype(bf16)
        to_across(q).start()
        to_near(q).start()
        return carry

    lax.fori_loop(0, peers, normalise, 0)

    def to_core(s, j):
        return pltpu.make_async_remote_copy(
            src_ref=gath.at[s, :, cols],
            dst_ref=gath.at[s, :, cols],
            send_sem=msend.at[s, j],
            recv_sem=mrecv.at[s, j],
            device_id={"mp": lax.rem(core + j, mp)},
            device_id_type=MESH,
        )

    def complete(s):
        for j in range(1, mp):
            to_core(s, j).start()

    def block(s, carry):
        @pl.when(s > 0)
        def _():
            for j in range(1, mp):
                to_core(s, j).wait_recv()

        kind = jnp.minimum(s, 1)
        seen = rowm[kind]
        keys = jnp.dot(gath[s], wbuf[1], preferred_element_type=f32)

        @pl.when(s == 0)
        def _():
            kown[...] = keys
            q = jnp.dot(gath[0], wbuf[0], preferred_element_type=f32)
            q = q * (LOG2E * HEAD_DIM ** (-0.5))
            lane = lax.broadcasted_iota(jnp.int32, (rows, 2 * HEAD_DIM), 1)
            for h in range(heads):
                pair = q[:, h // 2 * 2 * HEAD_DIM : (h // 2 + 1) * 2 * HEAD_DIM]
                keep = (lane < HEAD_DIM) if h % 2 == 0 else (lane >= HEAD_DIM)
                qm[h] = jnp.where(keep, pair, 0.0).astype(bf16)

        kbuf[...] = jnp.where(colm[kind] > 0, keys, kown[...]).astype(bf16)
        turned = lax.dot_general(wvt[...], gath[s], NT, preferred_element_type=f32) * seen
        row = lax.broadcasted_iota(jnp.int32, (PAD - HEAD_DIM, rows), 0)
        extra = jnp.where(row == 0, jnp.broadcast_to(seen, row.shape), 0.0).astype(bf16)
        for h in range(heads):
            vbuf[h, :HEAD_DIM] = turned[h * HEAD_DIM : (h + 1) * HEAD_DIM].astype(bf16)
            vbuf[h, HEAD_DIM:] = extra

        def scores(h, c):
            span = slice(c * half, (c + 1) * half)
            value = lax.dot_general(
                kbuf[span, h // 2 * 2 * HEAD_DIM : (h // 2 + 1) * 2 * HEAD_DIM],
                qm[h],
                NT,
                preferred_element_type=f32,
            )
            sbuf[h % 2, span] = value
            return jnp.max(value.reshape(half // 8, 8, rows), axis=0)

        peak = jnp.maximum(scores(0, 0), scores(0, 1))
        for h in range(heads):
            old = top[h]
            new = jnp.maximum(old, jnp.max(peak, axis=0, keepdims=True))
            top[h] = new
            summed, after = None, None
            for c in range(2):
                if h + 1 < heads:
                    value = scores(h + 1, c)
                    after = value if after is None else jnp.maximum(after, value)
                span = slice(c * half, (c + 1) * half)
                ahead = jnp.exp2(sbuf[h % 2, span] - new).astype(bf16)
                value = jnp.dot(vbuf[h, :, span], ahead, preferred_element_type=f32)
                summed = value if summed is None else summed + value
            acc[h] = acc[h] * jnp.exp2(old - new) + summed
            peak = after
            if h == heads // 2 - 1:
                for c in range(1, peers):

                    @pl.when(s == c)
                    def _(c=c):
                        if c == 1:
                            arrived(c, NEAR)
                        if c == 3:
                            arrived(c, NEAR)
                        arrived_rest(c)
                        complete(c + 1)

        @pl.when(s == 0)
        def _():
            arrived(0, Y)
            forward(0).start()
            arrived(0, NEAR)
            relay(0).start()
            arrived(1, Y)
            forward(1).start()
            arrived(2, Y)
            forward(2).start()
            arrived(2, NEAR)
            relay(2).start()
            early(1)
            arrived(0, Z)
            arrived(0, RELAYED)
            complete(1)
            arrived(3, Y)
            forward(3).start()

        @pl.when(s == 1)
        def _():
            early(3)

        return carry

    def early(c):
        @pl.when(relay_place == Z)
        def _():
            arrived(c, Z)

        relay(c).start()

    def arrived_rest(c):
        if c % 2 == 0:
            arrived(c, Z)
        else:

            @pl.when(relay_place != Z)
            def _():
                arrived(c, Z)

        arrived(c, RELAYED)

    lax.fori_loop(0, blocks, block, 0)
    for h in range(heads):
        mix = acc[h]
        attb[h * HEAD_DIM : (h + 1) * HEAD_DIM] = mix[:HEAD_DIM] / mix[HEAD_DIM : HEAD_DIM + 1]
    total[...] = attb[...].T.astype(bf16)

    first = 1 - region * 2 // n

    def half_of(h):
        return first if h == 0 else 1 - first

    def span_of(h):
        return pl.ds(pl.multiple_of(half_of(h) * half, half), half)

    def product(h, m):
        at = pl.ds(pl.multiple_of(m * width, width), width)
        return jnp.dot(total[span_of(h)], wobuf[:, at], preferred_element_type=f32)

    def share(h, j):
        return pltpu.make_async_remote_copy(
            src_ref=out_part.at[h, j],
            dst_ref=in_part.at[h, j],
            send_sem=rsend.at[h, j],
            recv_sem=rrecv.at[h, j],
            device_id={"mp": lax.rem(core + j, mp)},
            device_id_type=MESH,
        )

    def give(k):
        return pltpu.make_async_remote_copy(
            src_ref=back.at[pl.ds(pl.multiple_of(k * cap, cap), cap)],
            dst_ref=mine_of(returned_ref),
            send_sem=bsend.at[k],
            recv_sem=brecv.at[region],
            device_id={"region": k},
            device_id_type=MESH,
        )

    for h in range(2):
        for j in range(1, mp):
            out_part[h, j] = product(h, lax.rem(core + j, mp))
            share(h, j).start()
        span = span_of(h)
        state[span] = xg[core, span].astype(f32) + product(h, core)
    for h in range(2):
        span = span_of(h)
        value = state[span]
        for j in range(1, mp):
            share(h, j).wait_recv()
            value += in_part[h, j]
        state[span] = value
        back[span] = value.astype(bf16)

        def go(k, carry, h=h):
            other = half_of(h) * (n // 2) + k

            @pl.when(other != region)
            def _():
                give(other).start()

            return carry

        lax.fori_loop(0, n // 2, go, 0)

    keep = pltpu.make_async_copy(mine_of(back), mine_of(returned_ref), local.at[1])
    keep.start()
    low = (state[...] - back[...].astype(f32)).astype(bf16)
    ordered[...] = jnp.dot(hot[...], back[...], preferred_element_type=f32) + jnp.dot(
        hot[...], low, preferred_element_type=f32
    )
    out = pltpu.make_async_copy(ordered, mesh_ref, local.at[2])
    out.start()

    def drain(k, carry):
        for j in range(2):

            @pl.when(j * (n // 2) + k != n // 2 + n // 4)
            def _(j=j):
                sow(j, k).wait_send()

        return carry

    lax.fori_loop(0, n // 2, drain, 0)
    for c in range(peers):
        for j in range(1, mp):
            x_to_core(c, j).wait_send()
            to_core(c + 1, j).wait_send()
        for copy in (to_near, to_across, forward, relay):
            copy(c).wait_send()
    for h in range(2):
        for j in range(1, mp):
            share(h, j).wait_send()
    keep.wait()

    def finish(k, carry):
        @pl.when(k != region)
        def _():
            give(k).wait_send()
            pltpu.make_async_remote_copy(
                src_ref=back.at[pl.ds(0, cap)],
                dst_ref=returned_ref.at[pl.ds(pl.multiple_of(k * cap, cap), cap)],
                send_sem=bsend.at[k],
                recv_sem=brecv.at[k],
                device_id={"region": partner},
                device_id_type=MESH,
            ).wait_recv()

        return carry

    lax.fori_loop(0, n, finish, 0)
    out.wait()


def window(grid, weight, slot, nodes, peer_mask, gain, w_qkv, w_out, n, mp, cid):
    count, width = grid.shape
    rows = nodes.shape[1] * nodes.shape[2]
    depth = w_qkv.shape[1]
    heads = width // HEAD_DIM
    peers = PEERS
    chunk = rows // peers
    blocks = 1 + peers
    half = rows // 2
    bf16, f32 = jnp.bfloat16, jnp.float32
    vmem = pl.BlockSpec(memory_space=pltpu.VMEM)
    far = pl.BlockSpec(memory_space=pl.ANY)
    scalar = pl.BlockSpec(memory_space=pltpu.SMEM)
    dma = pltpu.SemaphoreType.DMA
    return pl.pallas_call(
        functools.partial(window_kernel, n, mp),
        out_shape=(
            jax.ShapeDtypeStruct((rows, width), f32),
            jax.ShapeDtypeStruct((rows, width), bf16),
        ),
        in_specs=[far, vmem, vmem, vmem, scalar, vmem, far, far],
        out_specs=(far, vmem),
        scratch_shapes=[
            pltpu.VMEM((count, width), bf16),
            pltpu.VMEM((count, 8), f32),
            pltpu.VMEM((count, width), bf16),
            pltpu.VMEM((2, half, width), bf16),
            pltpu.VMEM((mp, rows, width), bf16),
            pltpu.VMEM((blocks, rows, mp * width), bf16),
            pltpu.VMEM((3, depth, width), bf16),
            pltpu.VMEM((width, depth), bf16),
            pltpu.VMEM((width, depth), bf16),
            pltpu.VMEM((rows, rows), bf16),
            pltpu.VMEM((2, 1, rows), f32),
            pltpu.VMEM((2, rows, 1), f32),
            pltpu.VMEM((heads, rows, 2 * HEAD_DIM), bf16),
            pltpu.VMEM((rows, width), f32),
            pltpu.VMEM((rows, width), bf16),
            pltpu.VMEM((heads, PAD, rows), bf16),
            pltpu.VMEM((2, rows, rows), f32),
            pltpu.VMEM((heads, PAD, rows), f32),
            pltpu.VMEM((heads, 1, rows), f32),
            pltpu.VMEM((width, rows), f32),
            pltpu.VMEM((2, mp, half, width), f32),
            pltpu.VMEM((2, mp, half, width), f32),
            pltpu.VMEM((rows, width), bf16),
            pltpu.VMEM((rows, width), f32),
            pltpu.VMEM((rows, width), bf16),
            pltpu.VMEM((rows, width), f32),
            dma((3,)),
            dma((peers,)),
            dma((2,)),
            dma((n,)),
            dma((n,)),
            dma((peers, mp)),
            dma((peers, mp)),
            dma((peers, peers)),
            dma((peers, peers)),
            dma((blocks, mp)),
            dma((blocks, mp)),
            dma((2, mp)),
            dma((2, mp)),
            dma((n,)),
            dma((n,)),
        ],
        compiler_params=pltpu.CompilerParams(
            collective_id=cid, has_side_effects=True, vmem_limit_bytes=60 * 1024 * 1024
        ),
    )(grid, weight, slot, nodes, peer_mask, gain, w_qkv, w_out)


def on_device(n, mp, grid, g2m_weight, g2m_slot, slot_node, peer_mask, norm_gain, w_qkv, w_out):
    mesh_state, returned = window(
        grid, g2m_weight[None, :], g2m_slot[None, :], slot_node, peer_mask, norm_gain[None, :],
        w_qkv, w_out, n, mp, 0,
    )
    slots = returned.shape[0]
    slot_hot = (g2m_slot[None, :] == jnp.arange(slots, dtype=jnp.int32)[:, None]).astype(
        jnp.bfloat16
    )
    gathered = jnp.dot(slot_hot.T, returned, preferred_element_type=jnp.float32)
    grid_out = (grid.astype(jnp.float32) + gathered).astype(jnp.bfloat16)
    return (mesh_state, grid_out)


def solution(mesh):
    return jax.shard_map(
        functools.partial(on_device, mesh.shape["region"], mesh.shape["mp"]),
        mesh=mesh,
        in_specs=(
            P("region", "mp"),
            P("region"),
            P("region"),
            P("region", None, None),
            P("region", None),
            P(),
            P(None, None, "mp"),
            P("mp", None),
        ),
        out_specs=(P("region", "mp"), P("region", "mp")),
        check_vma=False,
    )
```

```python
import functools

import jax
import jax.numpy as jnp
from jax import lax
from jax.experimental import pallas as pl
from jax.experimental.pallas import tpu as pltpu
from jax.sharding import PartitionSpec as P

HEAD_DIM = 64
PAD = 80
PEERS = 4
NEAR, Y, Z, RELAYED = range(PEERS)
MESH = pl.DeviceIdType.MESH
LOG2E = 1.4426950408889634
NT = (((1,), (1,)), ((), ()))


def window_kernel(
    n, mp, grid_ref, weight_ref, slot_ref, node_ref, peer_ref, gain_ref, w_ref, wo_ref,
    mesh_ref, returned_ref,
    points, wcol, scaled, part, xg, gath, wbuf, wobuf, wvt, hot, rowm,
    qm, kown, kbuf, vbuf, sbuf, acc, top, attb, out_part, in_part, total, state, back, ordered,
    local, gsem, wsem, asend, arecv, xsend, xrecv, psend, precv, msend, mrecv, rsend, rrecv,
    bsend, brecv,
):
    f32, bf16 = jnp.float32, jnp.bfloat16
    region = lax.axis_index("region")
    core = lax.axis_index("mp")
    count, width = points.shape
    rows = xg.shape[1]
    cap = rows // n
    heads = width // HEAD_DIM
    peers = PEERS
    chunk = rows // peers
    blocks = 1 + peers
    half = rows // 2
    piece = count // peers
    odd = lax.rem(region, 2)
    far = lax.rem(region // 2, 2)
    partner = region + 1 - 2 * odd
    second = lax.rem(region + 2 - 4 * odd + n, n)
    across = region + 2 - 4 * far
    beyond = lax.rem(region + 4 - 8 * far + n, n)
    relay_place = jnp.where(odd == far, Y, Z)
    cols = pl.ds(pl.multiple_of(core * width, width), width)

    loads = [
        pltpu.make_async_copy(
            grid_ref.at[pl.ds(k * piece, piece)], points.at[pl.ds(k * piece, piece)], gsem.at[k]
        )
        for k in range(peers)
    ]
    for load in loads:
        load.start()
    weights = [
        pltpu.make_async_copy(w_ref, wbuf, wsem.at[0]),
        pltpu.make_async_copy(wo_ref, wobuf, wsem.at[1]),
    ]
    for load in weights:
        load.start()

    barrier = pltpu.get_barrier_semaphore()

    def hello(d, carry):
        pl.semaphore_signal(
            barrier, inc=1, device_id={"region": lax.rem(region + d, n)}, device_id_type=MESH
        )
        return carry

    lax.fori_loop(1, n, hello, 0)
    for j in range(1, mp):
        pl.semaphore_signal(
            barrier, inc=1, device_id={"mp": lax.rem(core + j, mp)}, device_id_type=MESH
        )

    wcol[...] = jnp.broadcast_to(weight_ref[...], (8, count)).T
    for k in range(peers):
        loads[k].wait()
        span = slice(k * piece, (k + 1) * piece)
        scaled[span] = (wcol[span, 0:1] * points[span].astype(f32)).astype(bf16)

    def mine_of(ref):
        return ref.at[pl.ds(pl.multiple_of(region * cap, cap), cap)]

    def base_of(j):
        return region + n // 4 + j * (n // 2)

    def scatter(j):
        place = lax.broadcasted_iota(jnp.int32, (half, 1), 0)
        ids = lax.rem(place // cap + base_of(j), n) * cap + lax.rem(place, cap)
        part[j] = jnp.dot(
            jnp.where(ids == slot_ref[...], 1.0, 0.0).astype(bf16),
            scaled[...],
            preferred_element_type=f32,
        ).astype(bf16)

    def sow(j, k):
        return pltpu.make_async_remote_copy(
            src_ref=part.at[j, pl.ds(pl.multiple_of(k * cap, cap), cap)],
            dst_ref=mine_of(xg.at[core]),
            send_sem=asend.at[j * (n // 2) + k],
            recv_sem=arecv.at[region],
            device_id={"region": lax.rem(base_of(j) + k, n)},
            device_id_type=MESH,
        )

    def sow_all(j, lo, hi):
        def go(k, carry):
            sow(j, k).start()
            return carry

        lax.fori_loop(lo, hi, go, 0)

    scatter(0)
    pl.semaphore_wait(barrier, n - 1 + mp - 1)
    sow_all(0, 0, n // 2)
    scatter(1)
    sow_all(1, 0, n // 4)
    sow_all(1, n // 4 + 1, n // 2)
    own = pltpu.make_async_copy(
        part.at[1, pl.ds(n // 4 * cap, cap)], mine_of(xg.at[core]), local.at[0]
    )
    own.start()

    acc[...] = jnp.zeros_like(acc)
    top[...] = jnp.full_like(top, -1e30)
    seen = [peer_ref[0, i].astype(f32) for i in range(4)]
    shown = {
        Y: jnp.where(far == 0, seen[3], seen[0]),
        Z: jnp.where(far == 0, seen[0], seen[3]),
        NEAR: jnp.where(odd == 0, seen[2], seen[1]),
        RELAYED: jnp.where(odd == 0, seen[1], seen[2]),
    }
    rowm[0] = jnp.ones(rowm.shape[1:], f32)
    for p in range(peers):
        rowm[1 + p] = jnp.full(rowm.shape[1:], shown[p], f32)
    own.wait()

    group = region * peers // n
    turns = (
        group,
        group + 1 - 2 * lax.rem(group, 2),
        jnp.where(group < 2, 2, 1),
        jnp.where(group < 2, 3, 0),
    )

    def turn(c):
        return turns[c]

    def x_to_core(q, j):
        span = pl.ds(pl.multiple_of(q * chunk, chunk), chunk)
        return pltpu.make_async_remote_copy(
            src_ref=xg.at[core, span],
            dst_ref=xg.at[core, span],
            send_sem=xsend.at[q, j],
            recv_sem=xrecv.at[q, j],
            device_id={"mp": lax.rem(core + j, mp)},
            device_id_type=MESH,
        )

    def reap(c):
        q = turn(c)

        def one(k, carry):
            source = q * (n // peers) + k

            @pl.when(source != region)
            def _():
                pltpu.make_async_remote_copy(
                    src_ref=part.at[0, pl.ds(0, cap)],
                    dst_ref=xg.at[core, pl.ds(pl.multiple_of(source * cap, cap), cap)],
                    send_sem=asend.at[0],
                    recv_sem=arecv.at[source],
                    device_id={"region": partner},
                    device_id_type=MESH,
                ).wait_recv()

            return carry

        lax.fori_loop(0, n // peers, one, 0)
        for j in range(1, mp):
            x_to_core(q, j).start()

    def send(c, place, source, other):
        return pltpu.make_async_remote_copy(
            src_ref=source,
            dst_ref=gath.at[1 + place, pl.ds(c * chunk, chunk), cols],
            send_sem=psend.at[c, place],
            recv_sem=precv.at[c, place],
            device_id={"region": other},
            device_id_type=MESH,
        )

    def own_chunk(c):
        return gath.at[0, pl.ds(pl.multiple_of(turn(c) * chunk, chunk), chunk), cols]

    def held(c, place):
        return gath.at[1 + place, pl.ds(c * chunk, chunk), cols]

    def to_near(c):
        return send(c, NEAR, own_chunk(c), partner)

    def to_across(c):
        return send(c, Y, own_chunk(c), across)

    def forward(c):
        return send(c, Z, held(c, Y), beyond)

    def relay(c):
        if c >= peers - 1:
            return send(c, RELAYED, held(c, NEAR), second)
        return send(c, RELAYED, held(c, relay_place), partner)

    def arrived(c, place):
        pltpu.make_async_remote_copy(
            src_ref=own_chunk(0),
            dst_ref=held(c, place),
            send_sem=psend.at[c, place],
            recv_sem=precv.at[c, place],
            device_id={"region": partner},
            device_id_type=MESH,
        ).wait_recv()

    def normalise(c):
        q = turn(c)
        for j in range(1, mp):
            x_to_core(q, j).wait_recv()
        span = pl.ds(pl.multiple_of(q * chunk, chunk), chunk)
        square = jnp.zeros((chunk, 1), f32)
        for m in range(mp):
            value = xg[m, span].astype(f32)
            square += jnp.sum(value * value, axis=-1, keepdims=True)
        inv = lax.rsqrt(square / (mp * width) + 1e-05)
        for m in range(mp):
            at = slice(m * width, (m + 1) * width)
            gath[0, span, at] = (xg[m, span].astype(f32) * inv * gain_ref[:, at]).astype(bf16)
        to_across(c).start()
        to_near(c).start()

    for c in range(2):
        reap(c)
        normalise(c)
    lane = lax.broadcasted_iota(jnp.int32, (n, rows), 1)
    spread = jnp.zeros((n, rows), jnp.int32)
    for c in range(cap):
        spread = jnp.where(lax.rem(lane, cap) == c, node_ref[0, :, c : c + 1], spread)
    owner = lax.broadcasted_iota(jnp.int32, (n, rows), 0)
    flat = jnp.sum(jnp.where(lane // cap == owner, spread, 0), axis=0, keepdims=True)
    hot[...] = jnp.where(
        lax.broadcasted_iota(jnp.int32, (rows, rows), 0) == flat, 1.0, 0.0
    ).astype(bf16)
    for load in weights:
        load.wait()
    wvt[...] = wbuf[2].T
    arrived(0, Y)
    forward(0).start()
    reap(2)
    normalise(2)
    arrived(1, Y)
    forward(1).start()
    reap(3)
    normalise(3)
    arrived(2, Y)
    forward(2).start()

    def to_core(s, j):
        return pltpu.make_async_remote_copy(
            src_ref=gath.at[s, :, cols],
            dst_ref=gath.at[s, :, cols],
            send_sem=msend.at[s, j],
            recv_sem=mrecv.at[s, j],
            device_id={"mp": lax.rem(core + j, mp)},
            device_id_type=MESH,
        )

    def complete(s):
        for j in range(1, mp):
            to_core(s, j).start()

    def block(s, carry):
        @pl.when(s > 0)
        def _():
            for j in range(1, mp):
                to_core(s, j).wait_recv()

        seen = rowm[s, :, :rows]
        keys = jnp.dot(gath[s], wbuf[1], preferred_element_type=f32)

        @pl.when(s == 0)
        def _():
            kown[...] = keys
            q = jnp.dot(gath[0], wbuf[0], preferred_element_type=f32)
            q = q * (LOG2E * HEAD_DIM ** (-0.5))
            lane = lax.broadcasted_iota(jnp.int32, (rows, 2 * HEAD_DIM), 1)
            for h in range(heads):
                pair = q[:, h // 2 * 2 * HEAD_DIM : (h // 2 + 1) * 2 * HEAD_DIM]
                keep = (lane < HEAD_DIM) if h % 2 == 0 else (lane >= HEAD_DIM)
                qm[h] = jnp.where(keep, pair, 0.0).astype(bf16)

        kbuf[...] = jnp.where(rowm[s, :, :width] > 0, keys, kown[...]).astype(bf16)
        turned = lax.dot_general(wvt[...], gath[s], NT, preferred_element_type=f32) * seen
        row = lax.broadcasted_iota(jnp.int32, (PAD - HEAD_DIM, rows), 0)
        extra = jnp.where(row == 0, jnp.broadcast_to(seen, row.shape), 0.0).astype(bf16)
        for h in range(heads):
            vbuf[h, :HEAD_DIM] = turned[h * HEAD_DIM : (h + 1) * HEAD_DIM].astype(bf16)
            vbuf[h, HEAD_DIM:] = extra

        def scores(h, c):
            span = slice(c * half, (c + 1) * half)
            value = lax.dot_general(
                kbuf[span, h // 2 * 2 * HEAD_DIM : (h // 2 + 1) * 2 * HEAD_DIM],
                qm[h],
                NT,
                preferred_element_type=f32,
            )
            sbuf[h % 2, span] = value
            return jnp.max(value.reshape(half // 8, 8, rows), axis=0)

        peak = jnp.maximum(scores(0, 0), scores(0, 1))
        for h in range(heads):
            old = top[h]
            new = jnp.maximum(old, jnp.max(peak, axis=0, keepdims=True))
            top[h] = new
            summed, after = None, None
            for c in range(2):
                if h + 1 < heads:
                    value = scores(h + 1, c)
                    after = value if after is None else jnp.maximum(after, value)
                span = slice(c * half, (c + 1) * half)
                ahead = jnp.exp2(sbuf[h % 2, span] - new).astype(bf16)
                value = jnp.dot(vbuf[h, :, span], ahead, preferred_element_type=f32)
                summed = value if summed is None else summed + value
            acc[h] = acc[h] * jnp.exp2(old - new) + summed
            peak = after
            if h == max(heads // 2 - 1, 0):

                @pl.when(s == 0)
                def _():
                    for c in range(3, peers):
                        arrived(c, Y)
                        forward(c).start()
                    for c in range(peers):
                        arrived(c, NEAR)
                        if c >= peers - 1:
                            relay(c).start()
                    complete(1 + NEAR)
                    complete(1 + Y)

                @pl.when(s == 1)
                def _():
                    early(2)

                @pl.when(s == 2)
                def _():
                    for c in range(peers):
                        if c < peers - 1:
                            late(c)
                        else:
                            arrived(c, Z)
                    complete(1 + Z)

                @pl.when(s == 3)
                def _():
                    for c in range(peers):
                        arrived(c, RELAYED)
                    complete(1 + RELAYED)

        @pl.when(s == 0)
        def _():
            early(0)
            early(1)

        return carry

    def early(c):
        @pl.when(relay_place == Z)
        def _():
            arrived(c, Z)

        relay(c).start()

    def late(c):
        @pl.when(relay_place != Z)
        def _():
            arrived(c, Z)

    lax.fori_loop(0, blocks, block, 0)
    for h in range(heads):
        mix = acc[h]
        attb[h * HEAD_DIM : (h + 1) * HEAD_DIM] = mix[:HEAD_DIM] / mix[HEAD_DIM : HEAD_DIM + 1]
    total[...] = attb[...].T.astype(bf16)

    first = 1 - region * 2 // n

    def half_of(h):
        return first if h == 0 else 1 - first

    def span_of(h):
        return pl.ds(pl.multiple_of(half_of(h) * half, half), half)

    def product(h, m):
        at = pl.ds(pl.multiple_of(m * width, width), width)
        return jnp.dot(total[span_of(h)], wobuf[:, at], preferred_element_type=f32)

    def share(h, j):
        return pltpu.make_async_remote_copy(
            src_ref=out_part.at[h, j],
            dst_ref=in_part.at[h, j],
            send_sem=rsend.at[h, j],
            recv_sem=rrecv.at[h, j],
            device_id={"mp": lax.rem(core + j, mp)},
            device_id_type=MESH,
        )

    def give(k):
        return pltpu.make_async_remote_copy(
            src_ref=back.at[pl.ds(pl.multiple_of(k * cap, cap), cap)],
            dst_ref=mine_of(returned_ref),
            send_sem=bsend.at[k],
            recv_sem=brecv.at[region],
            device_id={"region": k},
            device_id_type=MESH,
        )

    for h in range(2):
        for j in range(1, mp):
            out_part[h, j] = product(h, lax.rem(core + j, mp))
            share(h, j).start()
        span = span_of(h)
        state[span] = xg[core, span].astype(f32) + product(h, core)
    for h in range(2):
        span = span_of(h)
        value = state[span]
        for j in range(1, mp):
            share(h, j).wait_recv()
            value += in_part[h, j]
        state[span] = value
        back[span] = value.astype(bf16)

        def go(k, carry, h=h):
            other = half_of(h) * (n // 2) + k

            @pl.when(other != region)
            def _():
                give(other).start()

            return carry

        lax.fori_loop(0, n // 2, go, 0)

    keep = pltpu.make_async_copy(mine_of(back), mine_of(returned_ref), local.at[1])
    keep.start()
    low = (state[...] - back[...].astype(f32)).astype(bf16)
    ordered[...] = jnp.dot(hot[...], back[...], preferred_element_type=f32) + jnp.dot(
        hot[...], low, preferred_element_type=f32
    )
    out = pltpu.make_async_copy(ordered, mesh_ref, local.at[2])
    out.start()

    def drain(k, carry):
        for j in range(2):

            @pl.when(j * (n // 2) + k != n // 2 + n // 4)
            def _(j=j):
                sow(j, k).wait_send()

        return carry

    lax.fori_loop(0, n // 2, drain, 0)
    for c in range(peers):
        for j in range(1, mp):
            x_to_core(c, j).wait_send()
            to_core(c + 1, j).wait_send()
        for copy in (to_near, to_across, forward, relay):
            copy(c).wait_send()
    for h in range(2):
        for j in range(1, mp):
            share(h, j).wait_send()
    keep.wait()

    def finish(k, carry):
        @pl.when(k != region)
        def _():
            give(k).wait_send()
            pltpu.make_async_remote_copy(
                src_ref=back.at[pl.ds(0, cap)],
                dst_ref=returned_ref.at[pl.ds(pl.multiple_of(k * cap, cap), cap)],
                send_sem=bsend.at[k],
                recv_sem=brecv.at[k],
                device_id={"region": partner},
                device_id_type=MESH,
            ).wait_recv()

        return carry

    lax.fori_loop(0, n, finish, 0)
    out.wait()


def window(grid, weight, slot, nodes, peer_mask, gain, w_qkv, w_out, n, mp, cid):
    count, width = grid.shape
    rows = nodes.shape[1] * nodes.shape[2]
    depth = w_qkv.shape[1]
    heads = width // HEAD_DIM
    peers = PEERS
    chunk = rows // peers
    blocks = 1 + peers
    half = rows // 2
    bf16, f32 = jnp.bfloat16, jnp.float32
    vmem = pl.BlockSpec(memory_space=pltpu.VMEM)
    far = pl.BlockSpec(memory_space=pl.ANY)
    scalar = pl.BlockSpec(memory_space=pltpu.SMEM)
    dma = pltpu.SemaphoreType.DMA
    return pl.pallas_call(
        functools.partial(window_kernel, n, mp),
        out_shape=(
            jax.ShapeDtypeStruct((rows, width), f32),
            jax.ShapeDtypeStruct((rows, width), bf16),
        ),
        in_specs=[far, vmem, vmem, vmem, scalar, vmem, far, far],
        out_specs=(far, vmem),
        scratch_shapes=[
            pltpu.VMEM((count, width), bf16),
            pltpu.VMEM((count, 8), f32),
            pltpu.VMEM((count, width), bf16),
            pltpu.VMEM((2, half, width), bf16),
            pltpu.VMEM((mp, rows, width), bf16),
            pltpu.VMEM((blocks, rows, mp * width), bf16),
            pltpu.VMEM((3, depth, width), bf16),
            pltpu.VMEM((width, depth), bf16),
            pltpu.VMEM((width, depth), bf16),
            pltpu.VMEM((rows, rows), bf16),
            pltpu.VMEM((blocks, 1, max(rows, width)), f32),
            pltpu.VMEM((heads, rows, 2 * HEAD_DIM), bf16),
            pltpu.VMEM((rows, width), f32),
            pltpu.VMEM((rows, width), bf16),
            pltpu.VMEM((heads, PAD, rows), bf16),
            pltpu.VMEM((2, rows, rows), f32),
            pltpu.VMEM((heads, PAD, rows), f32),
            pltpu.VMEM((heads, 1, rows), f32),
            pltpu.VMEM((width, rows), f32),
            pltpu.VMEM((2, mp, half, width), f32),
            pltpu.VMEM((2, mp, half, width), f32),
            pltpu.VMEM((rows, width), bf16),
            pltpu.VMEM((rows, width), f32),
            pltpu.VMEM((rows, width), bf16),
            pltpu.VMEM((rows, width), f32),
            dma((3,)),
            dma((peers,)),
            dma((2,)),
            dma((n,)),
            dma((n,)),
            dma((peers, mp)),
            dma((peers, mp)),
            dma((peers, peers)),
            dma((peers, peers)),
            dma((blocks, mp)),
            dma((blocks, mp)),
            dma((2, mp)),
            dma((2, mp)),
            dma((n,)),
            dma((n,)),
        ],
        compiler_params=pltpu.CompilerParams(
            collective_id=cid, has_side_effects=True, vmem_limit_bytes=60 * 1024 * 1024
        ),
    )(grid, weight, slot, nodes, peer_mask, gain, w_qkv, w_out)


def on_device(n, mp, grid, g2m_weight, g2m_slot, slot_node, peer_mask, norm_gain, w_qkv, w_out):
    mesh_state, returned = window(
        grid, g2m_weight[None, :], g2m_slot[None, :], slot_node, peer_mask, norm_gain[None, :],
        w_qkv, w_out, n, mp, 0,
    )
    slots = returned.shape[0]
    slot_hot = (g2m_slot[None, :] == jnp.arange(slots, dtype=jnp.int32)[:, None]).astype(
        jnp.bfloat16
    )
    gathered = jnp.dot(slot_hot.T, returned, preferred_element_type=jnp.float32)
    grid_out = (grid.astype(jnp.float32) + gathered).astype(jnp.bfloat16)
    return (mesh_state, grid_out)


def solution(mesh):
    return jax.shard_map(
        functools.partial(on_device, mesh.shape["region"], mesh.shape["mp"]),
        mesh=mesh,
        in_specs=(
            P("region", "mp"),
            P("region"),
            P("region"),
            P("region", None, None),
            P("region", None),
            P(),
            P(None, None, "mp"),
            P("mp", None),
        ),
        out_specs=(P("region", "mp"), P("region", "mp")),
        check_vma=False,
    )
```

```python
import functools

import jax
import jax.numpy as jnp
from jax import lax
from jax.experimental import pallas as pl
from jax.experimental.pallas import tpu as pltpu
from jax.sharding import PartitionSpec as P

HEAD_DIM = 64
PAD = 80
PEERS = 4
NEAR, Y, Z, RELAYED = range(PEERS)
MESH = pl.DeviceIdType.MESH
LOG2E = 1.4426950408889634
NT = (((1,), (1,)), ((), ()))


def window_kernel(
    n, mp, grid_ref, weight_ref, slot_ref, node_ref, peer_ref, gain_ref, w_ref, wo_ref,
    mesh_ref, returned_ref,
    points, wcol, scaled, part, xg, gath, wbuf, wobuf, wvt, hot, rowm,
    qm, kown, kbuf, vbuf, sbuf, acc, top, attb, out_part, in_part, total, state, back, ordered,
    local, gsem, wsem, asend, arecv, xsend, xrecv, psend, precv, msend, mrecv, rsend, rrecv,
    bsend, brecv,
):
    f32, bf16 = jnp.float32, jnp.bfloat16
    region = lax.axis_index("region")
    core = lax.axis_index("mp")
    count, width = points.shape
    rows = xg.shape[1]
    cap = rows // n
    heads = width // HEAD_DIM
    peers = PEERS
    chunk = rows // peers
    blocks = 1 + peers
    half = rows // 2
    piece = count // peers
    odd = lax.rem(region, 2)
    far = lax.rem(region // 2, 2)
    partner = region + 1 - 2 * odd
    second = lax.rem(region + 2 - 4 * odd + n, n)
    across = region + 2 - 4 * far
    beyond = lax.rem(region + 4 - 8 * far + n, n)
    relay_place = jnp.where(odd == far, Y, Z)
    cols = pl.ds(pl.multiple_of(core * width, width), width)

    loads = [
        pltpu.make_async_copy(
            grid_ref.at[pl.ds(k * piece, piece)], points.at[pl.ds(k * piece, piece)], gsem.at[k]
        )
        for k in range(peers)
    ]
    for load in loads:
        load.start()
    weights = [
        pltpu.make_async_copy(w_ref, wbuf, wsem.at[0]),
        pltpu.make_async_copy(wo_ref, wobuf, wsem.at[1]),
    ]
    for load in weights:
        load.start()

    barrier = pltpu.get_barrier_semaphore()

    def hello(d, carry):
        pl.semaphore_signal(
            barrier, inc=1, device_id={"region": lax.rem(region + d, n)}, device_id_type=MESH
        )
        return carry

    lax.fori_loop(1, n, hello, 0)
    for j in range(1, mp):
        pl.semaphore_signal(
            barrier, inc=1, device_id={"mp": lax.rem(core + j, mp)}, device_id_type=MESH
        )

    wcol[...] = jnp.broadcast_to(weight_ref[...], (8, count)).T
    for k in range(peers):
        loads[k].wait()
        span = slice(k * piece, (k + 1) * piece)
        scaled[span] = (wcol[span, 0:1] * points[span].astype(f32)).astype(bf16)

    def mine_of(ref):
        return ref.at[pl.ds(pl.multiple_of(region * cap, cap), cap)]

    def base_of(j):
        return region + n // 4 + j * (n // 2)

    def scatter(j):
        place = lax.broadcasted_iota(jnp.int32, (half, 1), 0)
        ids = lax.rem(place // cap + base_of(j), n) * cap + lax.rem(place, cap)
        part[j] = jnp.dot(
            jnp.where(ids == slot_ref[...], 1.0, 0.0).astype(bf16),
            scaled[...],
            preferred_element_type=f32,
        ).astype(bf16)

    def sow(j, k):
        return pltpu.make_async_remote_copy(
            src_ref=part.at[j, pl.ds(pl.multiple_of(k * cap, cap), cap)],
            dst_ref=mine_of(xg.at[core]),
            send_sem=asend.at[j * (n // 2) + k],
            recv_sem=arecv.at[region],
            device_id={"region": lax.rem(base_of(j) + k, n)},
            device_id_type=MESH,
        )

    def sow_all(j, lo, hi):
        def go(k, carry):
            sow(j, k).start()
            return carry

        lax.fori_loop(lo, hi, go, 0)

    scatter(0)
    pl.semaphore_wait(barrier, n - 1 + mp - 1)
    sow_all(0, 0, n // 2)
    scatter(1)
    sow_all(1, 0, n // 4)
    sow_all(1, n // 4 + 1, n // 2)
    own = pltpu.make_async_copy(
        part.at[1, pl.ds(n // 4 * cap, cap)], mine_of(xg.at[core]), local.at[0]
    )
    own.start()

    acc[...] = jnp.zeros_like(acc)
    top[...] = jnp.full_like(top, -1e30)
    seen = [peer_ref[0, i].astype(f32) for i in range(4)]
    shown = {
        Y: jnp.where(far == 0, seen[3], seen[0]),
        Z: jnp.where(far == 0, seen[0], seen[3]),
        NEAR: jnp.where(odd == 0, seen[2], seen[1]),
        RELAYED: jnp.where(odd == 0, seen[1], seen[2]),
    }
    rowm[0] = jnp.ones(rowm.shape[1:], f32)
    for p in range(peers):
        rowm[1 + p] = jnp.full(rowm.shape[1:], shown[p], f32)
    own.wait()

    group = region * peers // n
    turns = (
        group,
        group + 1 - 2 * lax.rem(group, 2),
        jnp.where(group < 2, 2, 1),
        jnp.where(group < 2, 3, 0),
    )

    def turn(c):
        return turns[c]

    def x_to_core(q, j):
        span = pl.ds(pl.multiple_of(q * chunk, chunk), chunk)
        return pltpu.make_async_remote_copy(
            src_ref=xg.at[core, span],
            dst_ref=xg.at[core, span],
            send_sem=xsend.at[q, j],
            recv_sem=xrecv.at[q, j],
            device_id={"mp": lax.rem(core + j, mp)},
            device_id_type=MESH,
        )

    def reap(c):
        q = turn(c)

        def one(k, carry):
            source = q * (n // peers) + k

            @pl.when(source != region)
            def _():
                pltpu.make_async_remote_copy(
                    src_ref=part.at[0, pl.ds(0, cap)],
                    dst_ref=xg.at[core, pl.ds(pl.multiple_of(source * cap, cap), cap)],
                    send_sem=asend.at[0],
                    recv_sem=arecv.at[source],
                    device_id={"region": partner},
                    device_id_type=MESH,
                ).wait_recv()

            return carry

        lax.fori_loop(0, n // peers, one, 0)
        for j in range(1, mp):
            x_to_core(q, j).start()

    def send(c, place, source, other):
        return pltpu.make_async_remote_copy(
            src_ref=source,
            dst_ref=gath.at[1 + place, pl.ds(c * chunk, chunk), cols],
            send_sem=psend.at[c, place],
            recv_sem=precv.at[c, place],
            device_id={"region": other},
            device_id_type=MESH,
        )

    def own_chunk(c):
        return gath.at[0, pl.ds(pl.multiple_of(turn(c) * chunk, chunk), chunk), cols]

    def held(c, place):
        return gath.at[1 + place, pl.ds(c * chunk, chunk), cols]

    def to_near(c):
        return send(c, NEAR, own_chunk(c), partner)

    def to_across(c):
        return send(c, Y, own_chunk(c), across)

    def forward(c):
        return send(c, Z, held(c, Y), beyond)

    def relay(c):
        if c >= peers - 1:
            return send(c, RELAYED, held(c, NEAR), second)
        return send(c, RELAYED, held(c, relay_place), partner)

    def arrived(c, place):
        pltpu.make_async_remote_copy(
            src_ref=own_chunk(0),
            dst_ref=held(c, place),
            send_sem=psend.at[c, place],
            recv_sem=precv.at[c, place],
            device_id={"region": partner},
            device_id_type=MESH,
        ).wait_recv()

    def normalise(c):
        q = turn(c)
        for j in range(1, mp):
            x_to_core(q, j).wait_recv()
        span = pl.ds(pl.multiple_of(q * chunk, chunk), chunk)
        square = jnp.zeros((chunk, 1), f32)
        for m in range(mp):
            value = xg[m, span].astype(f32)
            square += jnp.sum(value * value, axis=-1, keepdims=True)
        inv = lax.rsqrt(square / (mp * width) + 1e-05)
        for m in range(mp):
            at = slice(m * width, (m + 1) * width)
            gath[0, span, at] = (xg[m, span].astype(f32) * inv * gain_ref[:, at]).astype(bf16)
        to_across(c).start()
        to_near(c).start()

    for c in range(2):
        reap(c)
        normalise(c)
    lane = lax.broadcasted_iota(jnp.int32, (n, rows), 1)
    spread = jnp.zeros((n, rows), jnp.int32)
    for c in range(cap):
        spread = jnp.where(lax.rem(lane, cap) == c, node_ref[0, :, c : c + 1], spread)
    owner = lax.broadcasted_iota(jnp.int32, (n, rows), 0)
    flat = jnp.sum(jnp.where(lane // cap == owner, spread, 0), axis=0, keepdims=True)
    hot[...] = jnp.where(
        lax.broadcasted_iota(jnp.int32, (rows, rows), 0) == flat, 1.0, 0.0
    ).astype(bf16)
    for load in weights:
        load.wait()
    wvt[...] = wbuf[2].T
    arrived(0, Y)
    forward(0).start()
    reap(2)
    normalise(2)
    arrived(1, Y)
    forward(1).start()
    reap(3)
    normalise(3)
    arrived(2, Y)
    forward(2).start()

    def to_core(s, j):
        return pltpu.make_async_remote_copy(
            src_ref=gath.at[s, :, cols],
            dst_ref=gath.at[s, :, cols],
            send_sem=msend.at[s, j],
            recv_sem=mrecv.at[s, j],
            device_id={"mp": lax.rem(core + j, mp)},
            device_id_type=MESH,
        )

    def complete(s):
        for j in range(1, mp):
            to_core(s, j).start()

    def block(s, carry):
        @pl.when(s > 0)
        def _():
            for j in range(1, mp):
                to_core(s, j).wait_recv()

        seen = rowm[s, :, :rows]
        keys = jnp.dot(gath[s], wbuf[1], preferred_element_type=f32)

        @pl.when(s == 0)
        def _():
            kown[...] = keys
            q = jnp.dot(gath[0], wbuf[0], preferred_element_type=f32)
            q = q * (LOG2E * HEAD_DIM ** (-0.5))
            lane = lax.broadcasted_iota(jnp.int32, (rows, 2 * HEAD_DIM), 1)
            for h in range(heads):
                pair = q[:, h // 2 * 2 * HEAD_DIM : (h // 2 + 1) * 2 * HEAD_DIM]
                keep = (lane < HEAD_DIM) if h % 2 == 0 else (lane >= HEAD_DIM)
                qm[h] = jnp.where(keep, pair, 0.0).astype(bf16)

        kbuf[...] = jnp.where(rowm[s, :, :width] > 0, keys, kown[...]).astype(bf16)
        turned = lax.dot_general(wvt[...], gath[s], NT, preferred_element_type=f32) * seen
        row = lax.broadcasted_iota(jnp.int32, (PAD - HEAD_DIM, rows), 0)
        extra = jnp.where(row == 0, jnp.broadcast_to(seen, row.shape), 0.0).astype(bf16)
        for h in range(heads):
            vbuf[h, :HEAD_DIM] = turned[h * HEAD_DIM : (h + 1) * HEAD_DIM].astype(bf16)
            vbuf[h, HEAD_DIM:] = extra

        def scores(h, c):
            span = slice(c * half, (c + 1) * half)
            value = lax.dot_general(
                kbuf[span, h // 2 * 2 * HEAD_DIM : (h // 2 + 1) * 2 * HEAD_DIM],
                qm[h],
                NT,
                preferred_element_type=f32,
            )
            sbuf[h % 2, span] = value
            return jnp.max(value.reshape(half // 8, 8, rows), axis=0)

        peak = jnp.maximum(scores(0, 0), scores(0, 1))
        for h in range(heads):
            old = top[h]
            new = jnp.maximum(old, jnp.max(peak, axis=0, keepdims=True))
            top[h] = new
            summed, after = None, None
            for c in range(2):
                if h + 1 < heads:
                    value = scores(h + 1, c)
                    after = value if after is None else jnp.maximum(after, value)
                span = slice(c * half, (c + 1) * half)
                ahead = jnp.exp2(sbuf[h % 2, span] - new).astype(bf16)
                value = jnp.dot(vbuf[h, :, span], ahead, preferred_element_type=f32)
                summed = value if summed is None else summed + value
            acc[h] = acc[h] * jnp.exp2(old - new) + summed
            peak = after
            if h == max(heads // 2 - 1, 0):

                @pl.when(s == 0)
                def _():
                    for c in range(3, peers):
                        arrived(c, Y)
                        forward(c).start()
                    for c in range(peers):
                        arrived(c, NEAR)
                        if c >= peers - 1:
                            relay(c).start()
                    complete(1 + NEAR)
                    complete(1 + Y)

                @pl.when(s == 1)
                def _():
                    early(2)

                @pl.when(s == 2)
                def _():
                    for c in range(peers):
                        if c < peers - 1:
                            late(c)
                        else:
                            arrived(c, Z)
                    complete(1 + Z)

                @pl.when(s == 3)
                def _():
                    for c in range(peers):
                        arrived(c, RELAYED)
                    complete(1 + RELAYED)

        @pl.when(s == 0)
        def _():
            early(0)
            early(1)

        return carry

    def early(c):
        @pl.when(relay_place == Z)
        def _():
            arrived(c, Z)

        relay(c).start()

    def late(c):
        @pl.when(relay_place != Z)
        def _():
            arrived(c, Z)

    lax.fori_loop(0, blocks, block, 0)
    for h in range(heads):
        mix = acc[h]
        attb[h * HEAD_DIM : (h + 1) * HEAD_DIM] = mix[:HEAD_DIM] / mix[HEAD_DIM : HEAD_DIM + 1]
    total[...] = attb[...].T.astype(bf16)

    first = 1 - region * 2 // n

    def half_of(h):
        return first if h == 0 else 1 - first

    def span_of(h):
        return pl.ds(pl.multiple_of(half_of(h) * half, half), half)

    def product(h, m):
        at = pl.ds(pl.multiple_of(m * width, width), width)
        return jnp.dot(total[span_of(h)], wobuf[:, at], preferred_element_type=f32)

    def share(h, j):
        return pltpu.make_async_remote_copy(
            src_ref=out_part.at[h, j],
            dst_ref=in_part.at[h, j],
            send_sem=rsend.at[h, j],
            recv_sem=rrecv.at[h, j],
            device_id={"mp": lax.rem(core + j, mp)},
            device_id_type=MESH,
        )

    def give(k):
        return pltpu.make_async_remote_copy(
            src_ref=back.at[pl.ds(pl.multiple_of(k * cap, cap), cap)],
            dst_ref=mine_of(returned_ref),
            send_sem=bsend.at[k],
            recv_sem=brecv.at[region],
            device_id={"region": k},
            device_id_type=MESH,
        )

    for h in range(2):
        for j in range(1, mp):
            out_part[h, j] = product(h, lax.rem(core + j, mp))
            share(h, j).start()
    for h in range(2):
        span = span_of(h)
        value = xg[core, span].astype(f32) + product(h, core)
        for j in range(1, mp):
            share(h, j).wait_recv()
            value += in_part[h, j]
        state[span] = value
        back[span] = value.astype(bf16)

        def go(k, carry, h=h):
            other = half_of(h) * (n // 2) + k

            @pl.when(other != region)
            def _():
                give(other).start()

            return carry

        lax.fori_loop(0, n // 2, go, 0)

    keep = pltpu.make_async_copy(mine_of(back), mine_of(returned_ref), local.at[1])
    keep.start()
    low = (state[...] - back[...].astype(f32)).astype(bf16)
    ordered[...] = jnp.dot(hot[...], back[...], preferred_element_type=f32) + jnp.dot(
        hot[...], low, preferred_element_type=f32
    )
    out = pltpu.make_async_copy(ordered, mesh_ref, local.at[2])
    out.start()

    def drain(k, carry):
        for j in range(2):

            @pl.when(j * (n // 2) + k != n // 2 + n // 4)
            def _(j=j):
                sow(j, k).wait_send()

        return carry

    lax.fori_loop(0, n // 2, drain, 0)
    for c in range(peers):
        for j in range(1, mp):
            x_to_core(c, j).wait_send()
            to_core(c + 1, j).wait_send()
        for copy in (to_near, to_across, forward, relay):
            copy(c).wait_send()
    for h in range(2):
        for j in range(1, mp):
            share(h, j).wait_send()
    keep.wait()

    def finish(k, carry):
        @pl.when(k != region)
        def _():
            give(k).wait_send()
            pltpu.make_async_remote_copy(
                src_ref=back.at[pl.ds(0, cap)],
                dst_ref=returned_ref.at[pl.ds(pl.multiple_of(k * cap, cap), cap)],
                send_sem=bsend.at[k],
                recv_sem=brecv.at[k],
                device_id={"region": partner},
                device_id_type=MESH,
            ).wait_recv()

        return carry

    lax.fori_loop(0, n, finish, 0)
    out.wait()


def window(grid, weight, slot, nodes, peer_mask, gain, w_qkv, w_out, n, mp, cid):
    count, width = grid.shape
    rows = nodes.shape[1] * nodes.shape[2]
    depth = w_qkv.shape[1]
    heads = width // HEAD_DIM
    peers = PEERS
    chunk = rows // peers
    blocks = 1 + peers
    half = rows // 2
    bf16, f32 = jnp.bfloat16, jnp.float32
    vmem = pl.BlockSpec(memory_space=pltpu.VMEM)
    far = pl.BlockSpec(memory_space=pl.ANY)
    scalar = pl.BlockSpec(memory_space=pltpu.SMEM)
    dma = pltpu.SemaphoreType.DMA
    return pl.pallas_call(
        functools.partial(window_kernel, n, mp),
        out_shape=(
            jax.ShapeDtypeStruct((rows, width), f32),
            jax.ShapeDtypeStruct((rows, width), bf16),
        ),
        in_specs=[far, vmem, vmem, vmem, scalar, vmem, far, far],
        out_specs=(far, vmem),
        scratch_shapes=[
            pltpu.VMEM((count, width), bf16),
            pltpu.VMEM((count, 8), f32),
            pltpu.VMEM((count, width), bf16),
            pltpu.VMEM((2, half, width), bf16),
            pltpu.VMEM((mp, rows, width), bf16),
            pltpu.VMEM((blocks, rows, mp * width), bf16),
            pltpu.VMEM((3, depth, width), bf16),
            pltpu.VMEM((width, depth), bf16),
            pltpu.VMEM((width, depth), bf16),
            pltpu.VMEM((rows, rows), bf16),
            pltpu.VMEM((blocks, 1, max(rows, width)), f32),
            pltpu.VMEM((heads, rows, 2 * HEAD_DIM), bf16),
            pltpu.VMEM((rows, width), f32),
            pltpu.VMEM((rows, width), bf16),
            pltpu.VMEM((heads, PAD, rows), bf16),
            pltpu.VMEM((2, rows, rows), f32),
            pltpu.VMEM((heads, PAD, rows), f32),
            pltpu.VMEM((heads, 1, rows), f32),
            pltpu.VMEM((width, rows), f32),
            pltpu.VMEM((2, mp, half, width), f32),
            pltpu.VMEM((2, mp, half, width), f32),
            pltpu.VMEM((rows, width), bf16),
            pltpu.VMEM((rows, width), f32),
            pltpu.VMEM((rows, width), bf16),
            pltpu.VMEM((rows, width), f32),
            dma((3,)),
            dma((peers,)),
            dma((2,)),
            dma((n,)),
            dma((n,)),
            dma((peers, mp)),
            dma((peers, mp)),
            dma((peers, peers)),
            dma((peers, peers)),
            dma((blocks, mp)),
            dma((blocks, mp)),
            dma((2, mp)),
            dma((2, mp)),
            dma((n,)),
            dma((n,)),
        ],
        compiler_params=pltpu.CompilerParams(
            collective_id=cid, has_side_effects=True, vmem_limit_bytes=60 * 1024 * 1024
        ),
    )(grid, weight, slot, nodes, peer_mask, gain, w_qkv, w_out)


def on_device(n, mp, grid, g2m_weight, g2m_slot, slot_node, peer_mask, norm_gain, w_qkv, w_out):
    mesh_state, returned = window(
        grid, g2m_weight[None, :], g2m_slot[None, :], slot_node, peer_mask, norm_gain[None, :],
        w_qkv, w_out, n, mp, 0,
    )
    slots = returned.shape[0]
    slot_hot = (g2m_slot[None, :] == jnp.arange(slots, dtype=jnp.int32)[:, None]).astype(
        jnp.bfloat16
    )
    gathered = jnp.dot(slot_hot.T, returned, preferred_element_type=jnp.float32)
    grid_out = (grid.astype(jnp.float32) + gathered).astype(jnp.bfloat16)
    return (mesh_state, grid_out)


def solution(mesh):
    return jax.shard_map(
        functools.partial(on_device, mesh.shape["region"], mesh.shape["mp"]),
        mesh=mesh,
        in_specs=(
            P("region", "mp"),
            P("region"),
            P("region"),
            P("region", None, None),
            P("region", None),
            P(),
            P(None, None, "mp"),
            P("mp", None),
        ),
        out_specs=(P("region", "mp"), P("region", "mp")),
        check_vma=False,
    )
```
